32 devices in a mesh: shard: 8 (over z, x), width: 4 (over y, core).
Axes of the slice: x: 2, y: 2, z: 4, core: 2. Of those that a mesh axis runs over, the one named last changes fastest.
Arguments:
- w_gate: bfloat16 [2048, 8192], P('shard', 'width'), may hold values from -0.125 to 0.125
- low_gate: bfloat16 [2048, 64], P('shard'), may hold values from -0.125 to 0.125
- high_gate: bfloat16 [64, 8192], P(None, 'width'), may hold values from -0.75 to 0.75
- w_up: bfloat16 [2048, 8192], P('shard', 'width'), may hold values from -0.125 to 0.125
- low_up: bfloat16 [2048, 64], P('shard'), may hold values from -0.125 to 0.125
- high_up: bfloat16 [64, 8192], P(None, 'width'), may hold values from -0.75 to 0.75
- w_down: bfloat16 [8192, 2048], P('width', 'shard'), may hold values from -0.0625 to 0.0625
- low_down: bfloat16 [8192, 64], P('width'), may hold values from -0.0625 to 0.0625
- high_down: bfloat16 [64, 2048], P(None, 'shard'), may hold values from -0.75 to 0.75
- norm_train: float32 [2048], P(('shard', 'width')), may hold values from 0.25 to 1.75
- norm_step: float32 [2048], P(('shard', 'width')), may hold values from -0.3 to 0.3
Outputs:
- serve_gate: bfloat16 [8192, 2048], P('width')
- serve_up: bfloat16 [8192, 2048], P('width')
- serve_down: bfloat16 [2048, 8192], P(None, 'width')
- serve_norm: bfloat16 [2048], replicated
The draws below stay inside these ranges and needn't reach their ends.
All inputs are finite; a program needn't handle non-finite values.
Results may differ from the reference program's by a relative error of at most 0.001.
Values may be sent and summed in bfloat16 or wider, within the bound.
A program may use at most 128 MiB of HBM per device.

```python
import jax
import jax.numpy as jnp

D_MODEL = 2048
D_INNER = 8192
RANK = 64


def level_of(own_key, extent, cuts, smallest, largest):
    factor_of, own = 1.0, jax.random.fold_in(own_key, 6)
    for dim, shards_of in cuts:
        steps = jnp.exp(jax.random.uniform(jax.random.fold_in(own, dim), (shards_of,), jnp.float32, smallest / len(cuts), largest / len(cuts)))
        factor_of = factor_of * jnp.repeat(steps, extent[dim] // shards_of).reshape([-1 if axis == dim else 1 for axis in range(len(extent))])
    return factor_of


def gaussian(stream_key, extent, deviation, reach, pieces=(), dtype=jnp.bfloat16):
    drawn = deviation * jax.random.normal(stream_key, extent, jnp.float32)
    if pieces:
        drawn = drawn * level_of(stream_key, extent, pieces, -0.22, 0.18)
    return jnp.clip(drawn, -reach, reach).astype(dtype)


def setup_inputs(seed: int = 0) -> dict:
    key_list = jax.random.split(jax.random.key(seed), 12)
    w_gate = gaussian(key_list[0], (D_MODEL, D_INNER), D_MODEL ** -0.5, 0.125, ((0, 8), (1, 4)))
    low_gate = gaussian(key_list[1], (D_MODEL, RANK), D_MODEL ** -0.5, 0.125, ((0, 8),))
    high_gate = gaussian(key_list[2], (RANK, D_INNER), RANK ** -0.5, 0.75, ((1, 4),))
    w_up = gaussian(key_list[3], (D_MODEL, D_INNER), D_MODEL ** -0.5, 0.125, ((0, 8), (1, 4)))
    low_up = gaussian(key_list[4], (D_MODEL, RANK), D_MODEL ** -0.5, 0.125, ((0, 8),))
    high_up = gaussian(key_list[5], (RANK, D_INNER), RANK ** -0.5, 0.75, ((1, 4),))
    w_down = gaussian(key_list[6], (D_INNER, D_MODEL), D_INNER ** -0.5, 0.0625, ((0, 4), (1, 8)))
    low_down = gaussian(key_list[7], (D_INNER, RANK), D_INNER ** -0.5, 0.0625, ((0, 4),))
    high_down = gaussian(key_list[8], (RANK, D_MODEL), RANK ** -0.5, 0.75, ((1, 8),))
    norm_train = jnp.clip(1.0 + 0.15 * jax.random.normal(key_list[9], (D_MODEL,), jnp.float32), 0.25, 1.75)
    norm_step = jnp.clip(jax.random.uniform(key_list[10], (D_MODEL,), jnp.float32, -0.3, 0.3) * level_of(key_list[10], (D_MODEL,), ((0, 32),), -0.4, 0.0), -0.3, 0.3)
    return {"w_gate": w_gate, "low_gate": low_gate, "high_gate": high_gate, "w_up": w_up, "low_up": low_up, "high_up": high_up, "w_down": w_down, "low_down": low_down, "high_down": high_down, "norm_train": norm_train, "norm_step": norm_step}


mix_rate = 2.0


def reference(w_gate, low_gate, high_gate, w_up, low_up, high_up, w_down, low_down, high_down, norm_train, norm_step):
    fresh_gate = w_gate.astype(jnp.float32) + mix_rate * jnp.dot(low_gate, high_gate, preferred_element_type=jnp.float32)
    fresh_up = w_up.astype(jnp.float32) + mix_rate * jnp.dot(low_up, high_up, preferred_element_type=jnp.float32)
    fresh_down = w_down.astype(jnp.float32) + mix_rate * jnp.dot(low_down, high_down, preferred_element_type=jnp.float32)
    serve_gate = fresh_gate.T.astype(jnp.bfloat16)
    serve_up = fresh_up.T.astype(jnp.bfloat16)
    serve_down = fresh_down.T.astype(jnp.bfloat16)
    serve_norm = (norm_train + norm_step).astype(jnp.bfloat16)
    return serve_gate, serve_up, serve_down, serve_norm
```

```python
import functools

import jax
import jax.numpy as jnp
from jax import lax
from jax.experimental import pallas as pl
from jax.experimental.pallas import tpu as pltpu
from jax.sharding import PartitionSpec as P

mix_rate = 2.0
MESH = pl.DeviceIdType.MESH
X = 2


def merged(w, low, high):
    fresh = w.astype(jnp.float32) + mix_rate * jnp.dot(
        low, high, preferred_element_type=jnp.float32
    )
    return fresh.astype(jnp.bfloat16)


PIECES = ((0, 0), (1, 0), (2, 0), (0, 1), (1, 1), (2, 1))
LINE = tuple(range(len(PIECES) - 1))
PAIR = len(PIECES) - 1
UP, DOWN, SIDE = 0, 1, 2


def gather_kernel(
    shards, widths, gate, up, down, norm, o_gate, o_up, o_down, o_norm,
    send_sem, recv_sem, norm_send, norm_recv, own_sem,
):
    lines = shards // X
    me, w = lax.axis_index("shard"), lax.axis_index("width")
    z, x = me // X, me % X
    partner = z * X + (1 - x)
    blocks, outs = (gate, up, down), (o_gate, o_up, o_down)
    n_pieces = len(PIECES)

    def own(c):
        t, h = PIECES[c]
        ref = blocks[t]
        if t < 2:
            half = ref.shape[0] // 2
            return ref.at[pl.ds(h * half, half), :]
        half = ref.shape[1] // 2
        return ref.at[:, pl.ds(h * half, half)]

    def place(s, c):
        t, h = PIECES[c]
        ref, out = blocks[t], outs[t]
        if t < 2:
            half, wide = ref.shape[0] // 2, ref.shape[1]
            return out.at[pl.ds(h * half, half), pl.ds(pl.multiple_of(s * wide, wide), wide)]
        half, tall = ref.shape[1] // 2, ref.shape[0]
        return out.at[pl.ds(pl.multiple_of(s * tall, tall), tall), pl.ds(h * half, half)]

    def target(way):
        return {UP: me + X, DOWN: me - X, SIDE: partner}[way]

    sends = []

    def when(conds, fn):
        if conds is None:
            fn()
        else:
            pl.when(conds)(fn)

    def has(way):
        return {UP: z + 1 < lines, DOWN: z > 0, SIDE: None}[way]

    def both(a, b):
        if a is None:
            return b
        if b is None:
            return a
        return jnp.logical_and(a, b)

    def send(way, s, c, slot, cond, from_own=False):
        def make():
            return pltpu.make_async_remote_copy(
                src_ref=own(c) if from_own else place(s, c),
                dst_ref=place(s, c),
                send_sem=send_sem.at[way, slot],
                recv_sem=recv_sem.at[s * n_pieces + c],
                device_id=(target(way), w),
                device_id_type=MESH,
            )

        full = both(cond, has(way))
        when(full, lambda: make().start())
        sends.append((full, lambda: make().wait_send()))

    def arrive(s, c, cond=None):
        when(
            cond,
            lambda: pltpu.make_async_remote_copy(
                src_ref=place(s, c),
                dst_ref=place(s, c),
                send_sem=send_sem.at[0, 0],
                recv_sem=recv_sem.at[s * n_pieces + c],
                device_id=(partner, w),
                device_id_type=MESH,
            ).wait_recv(),
        )

    def norm_rows(first, count):
        return o_norm.at[pl.ds(first, count)]

    def norm_copy(src, first, count, sem, rsem, dev):
        return pltpu.make_async_remote_copy(
            src_ref=src, dst_ref=norm_rows(first, count), send_sem=norm_send.at[sem],
            recv_sem=norm_recv.at[rsem], device_id=dev, device_id_type=MESH,
        )

    barrier = pltpu.get_barrier_semaphore()
    peers = [lax.rem(w + k, widths) for k in range(1, widths)]
    for p in peers:
        pl.semaphore_signal(barrier, inc=1, device_id=(me, p), device_id_type=MESH)
    for way in (UP, DOWN, SIDE):
        when(
            has(way),
            lambda way=way: pl.semaphore_signal(
                barrier, inc=1, device_id=(target(way), w), device_id_type=MESH
            ),
        )
    inner = jnp.logical_and(z > 0, z + 1 < lines)
    pl.when(inner)(lambda: pl.semaphore_wait(barrier, widths + 2))
    ends = widths + (1 if lines > 1 else 0)
    pl.when(jnp.logical_not(inner))(lambda: pl.semaphore_wait(barrier, ends))

    send(SIDE, me, PAIR, PAIR, None, from_own=True)
    for c in LINE:
        send(UP, me, c, c, None, from_own=True)
        send(DOWN, me, c, c, None, from_own=True)
        send(SIDE, me, c, c, None, from_own=True)
    kept = [pltpu.make_async_copy(own(c), place(me, c), own_sem.at[c]) for c in range(n_pieces)]
    norm_own = pltpu.make_async_copy(norm, norm_rows(me * widths + w, 1), own_sem.at[n_pieces])
    for copy in kept:
        copy.start()
    norm_own.start()
    tile_of = lambda k: norm_copy(norm, me * widths + w, 1, k - 1, k - 1, (me, peers[k - 1]))
    for k in range(1, widths):
        tile_of(k).start()
    norm_own.wait()
    for k in range(1, widths):
        source = lax.rem(w + widths - k, widths)
        norm_copy(norm, me * widths + source, 1, k - 1, k - 1, (me, peers[k - 1])).wait_recv()
    side_at = widths - 1
    norm_side = lambda s: norm_copy(
        norm_rows(s * widths, widths), s * widths, widths, side_at, side_at, (partner, w)
    )
    norm_side(me).start()

    for d in range(1, lines):
        for c in LINE:
            for way, s, cond in (
                (UP, me - d * X, z >= d),
                (DOWN, me + d * X, z + d < lines),
            ):
                arrive(s, c, cond)
                slot = d * n_pieces + c
                send(way, s, c, slot, cond)
                send(SIDE, s, c, slot + (way * lines * n_pieces), cond)

    arrive(partner, PAIR)
    norm_side(partner).wait_recv()

    def norm_pair(way, plane):
        rows = X * widths
        at = widths + way * lines
        return norm_copy(
            norm_rows(plane * rows, rows), plane * rows, rows,
            at + (plane - z) * (1 - 2 * way) * -1, widths + plane, (target(way), w),
        )

    line_slot = 2 * lines * n_pieces
    for d in range(lines):
        for way, plane, cond in (
            (UP, z - d, z >= d),
            (DOWN, z + d, z + d < lines),
        ):
            if d == 0:
                cond = None
            for j in range(X):
                s = me if (d == 0 and j == 0) else (partner if d == 0 else plane * X + j)
                if d > 0:
                    arrive(s, PAIR, cond)
                send(way, s, PAIR, line_slot + d * X + j, cond, from_own=(d == 0 and j == 0))
            full = both(cond, has(way))
            if d > 0:
                when(cond, lambda way=way, plane=plane: norm_pair(way, plane).wait_recv())
            when(full, lambda way=way, plane=plane: norm_pair(way, plane).start())
            sends.append((full, lambda way=way, plane=plane: norm_pair(way, plane).wait_send()))

    for c in LINE:
        arrive(partner, c)
    for d in range(1, lines):
        for c in LINE:
            arrive(partner - d * X, c, z >= d)
            arrive(partner + d * X, c, z + d < lines)
    for copy in kept:
        copy.wait()
    for k in range(1, widths):
        tile_of(k).wait_send()
    norm_side(me).wait_send()
    for cond, wait in sends:
        when(cond, wait)


def gather_all(shards, widths, gate, up, down, norm):
    lines = shards // X
    n_pieces = len(PIECES)
    any_ = pl.BlockSpec(memory_space=pl.ANY)
    vmem = pl.BlockSpec(memory_space=pltpu.VMEM)
    wide = lambda b: jax.ShapeDtypeStruct((b.shape[0], shards * b.shape[1]), b.dtype)
    tall = lambda b: jax.ShapeDtypeStruct((shards * b.shape[0], b.shape[1]), b.dtype)
    return pl.pallas_call(
        functools.partial(gather_kernel, shards, widths),
        out_shape=(
            wide(gate), wide(up), tall(down),
            jax.ShapeDtypeStruct((shards * widths,) + norm.shape[1:], norm.dtype),
        ),
        in_specs=[vmem] * 4,
        out_specs=(any_,) * 4,
        scratch_shapes=[
            pltpu.SemaphoreType.DMA((3, 2 * lines * n_pieces + lines * X)),
            pltpu.SemaphoreType.DMA((shards * n_pieces,)),
            pltpu.SemaphoreType.DMA((widths + 2 * lines,)),
            pltpu.SemaphoreType.DMA((widths + lines,)),
            pltpu.SemaphoreType.DMA((n_pieces + 1,)),
        ],
        compiler_params=pltpu.CompilerParams(collective_id=0, has_side_effects=True),
    )(gate, up, down, norm)


def body(
    shards,
    widths,
    w_gate,
    low_gate,
    high_gate,
    w_up,
    low_up,
    high_up,
    w_down,
    low_down,
    high_down,
    norm_train,
    norm_step,
):
    gate = merged(w_gate, low_gate, high_gate)
    up = merged(w_up, low_up, high_up)
    down = merged(w_down, low_down, high_down)
    gain = norm_train + norm_step
    if shards % X or gate.shape[0] % 128 or down.shape[0] % 256 or gain.shape[0] > 128:
        gate, up, down = (
            lax.all_gather(gate, "shard", axis=0, tiled=True),
            lax.all_gather(up, "shard", axis=0, tiled=True),
            lax.all_gather(down, "shard", axis=1, tiled=True),
        )
        gain = lax.all_gather(gain.astype(jnp.bfloat16), ("shard", "width"), axis=0, tiled=True)
        return gate.T, up.T, down.T, gain
    count = gain.shape[0]
    tile = jnp.pad(gain.reshape(1, 1, count), ((0, 0), (0, 7), (0, 128 - count)))
    gate, up, down, tiles = gather_all(shards, widths, gate.T, up.T, down.T, tile)
    return gate, up, down, tiles[:, 0, :count].reshape(-1).astype(jnp.bfloat16)


def solution(mesh):
    return jax.shard_map(
        functools.partial(body, mesh.shape["shard"], mesh.shape["width"]),
        mesh=mesh,
        in_specs=(
            P("shard", "width"),
            P("shard", None),
            P(None, "width"),
            P("shard", "width"),
            P("shard", None),
            P(None, "width"),
            P("width", "shard"),
            P("width", None),
            P(None, "shard"),
            P(("shard", "width")),
            P(("shard", "width")),
        ),
        out_specs=(P("width", None), P("width", None), P(None, "width"), P()),
        check_vma=False,
    )
```

```python
import functools

import jax
import jax.numpy as jnp
from jax import lax
from jax.experimental import pallas as pl
from jax.experimental.pallas import tpu as pltpu
from jax.sharding import PartitionSpec as P

mix_rate = 2.0
MESH = pl.DeviceIdType.MESH
X = 2


def merged(w, low, high):
    fresh = w.astype(jnp.float32) + mix_rate * jnp.dot(
        low, high, preferred_element_type=jnp.float32
    )
    return fresh.astype(jnp.bfloat16)


PIECES = ((0, 0), (1, 0), (2, 0), (0, 1), (1, 1), (2, 1))
LINE = tuple(range(len(PIECES) - 1))
PAIR = len(PIECES) - 1
UP, DOWN, SIDE = 0, 1, 2
STRIP = 128


def gather_kernel(
    shards, widths, gate, up, down, norm, o_gate, o_up, o_down, o_norm,
    send_sem, recv_sem, norm_send, norm_recv, own_sem,
):
    lines = shards // X
    me, w = lax.axis_index("shard"), lax.axis_index("width")
    z, x = me // X, me % X
    partner = z * X + (1 - x)
    blocks, outs = (gate, up, down), (o_gate, o_up, o_down)
    n_pieces = len(PIECES)

    def own(c):
        t, h = PIECES[c]
        ref = blocks[t]
        if t < 2:
            half = ref.shape[0] // 2
            return ref.at[pl.ds(h * half, half), :]
        half = ref.shape[1] // 2
        return ref.at[:, pl.ds(h * half, half)]

    def place(s, c):
        t, h = PIECES[c]
        ref, out = blocks[t], outs[t]
        if t < 2:
            half, wide = ref.shape[0] // 2, ref.shape[1]
            return out.at[pl.ds(h * half, half), pl.ds(pl.multiple_of(s * wide, wide), wide)]
        half, tall = ref.shape[1] // 2, ref.shape[0]
        return out.at[pl.ds(pl.multiple_of(s * tall, tall), tall), pl.ds(h * half, half)]

    def target(way):
        return {UP: me + X, DOWN: me - X, SIDE: partner}[way]

    sends = []

    def when(conds, fn):
        if conds is None:
            fn()
        else:
            pl.when(conds)(fn)

    def has(way):
        return {UP: z + 1 < lines, DOWN: z > 0, SIDE: None}[way]

    def both(a, b):
        if a is None:
            return b
        if b is None:
            return a
        return jnp.logical_and(a, b)

    def send(way, s, c, slot, cond, from_own=False):
        def make():
            return pltpu.make_async_remote_copy(
                src_ref=own(c) if from_own else place(s, c),
                dst_ref=place(s, c),
                send_sem=send_sem.at[way, slot],
                recv_sem=recv_sem.at[s * n_pieces + c],
                device_id=(target(way), w),
                device_id_type=MESH,
            )

        full = both(cond, has(way))
        when(full, lambda: make().start())
        sends.append((full, lambda: make().wait_send()))

    def arrive(s, c, cond=None):
        when(
            cond,
            lambda: pltpu.make_async_remote_copy(
                src_ref=place(s, c),
                dst_ref=place(s, c),
                send_sem=send_sem.at[0, 0],
                recv_sem=recv_sem.at[s * n_pieces + c],
                device_id=(partner, w),
                device_id_type=MESH,
            ).wait_recv(),
        )

    def norm_rows(first, count):
        return o_norm.at[pl.ds(first, count)]

    def norm_copy(src, first, count, sem, rsem, dev):
        return pltpu.make_async_remote_copy(
            src_ref=src, dst_ref=norm_rows(first, count), send_sem=norm_send.at[sem],
            recv_sem=norm_recv.at[rsem], device_id=dev, device_id_type=MESH,
        )

    barrier = pltpu.get_barrier_semaphore()
    peers = [lax.rem(w + k, widths) for k in range(1, widths)]
    for p in peers:
        pl.semaphore_signal(barrier, inc=1, device_id=(me, p), device_id_type=MESH)
    for way in (UP, DOWN, SIDE):
        when(
            has(way),
            lambda way=way: pl.semaphore_signal(
                barrier, inc=1, device_id=(target(way), w), device_id_type=MESH
            ),
        )
    inner = jnp.logical_and(z > 0, z + 1 < lines)
    pl.when(inner)(lambda: pl.semaphore_wait(barrier, widths + 2))
    ends = widths + (1 if lines > 1 else 0)
    pl.when(jnp.logical_not(inner))(lambda: pl.semaphore_wait(barrier, ends))

    send(SIDE, me, PAIR, PAIR, None, from_own=True)
    for c in LINE:
        send(UP, me, c, c, None, from_own=True)
        send(DOWN, me, c, c, None, from_own=True)
        send(SIDE, me, c, c, None, from_own=True)
    norm_own = pltpu.make_async_copy(norm, norm_rows(me * widths + w, 1), own_sem.at[0])
    norm_own.start()
    tile_of = lambda k: norm_copy(norm, me * widths + w, 1, k - 1, k - 1, (me, peers[k - 1]))
    for k in range(1, widths):
        tile_of(k).start()
    norm_own.wait()
    for k in range(1, widths):
        source = lax.rem(w + widths - k, widths)
        norm_copy(norm, me * widths + source, 1, k - 1, k - 1, (me, peers[k - 1])).wait_recv()
    side_at = widths - 1
    norm_side = lambda s: norm_copy(
        norm_rows(s * widths, widths), s * widths, widths, side_at, side_at, (partner, w)
    )
    norm_side(me).start()

    wide, tall = gate.shape[1], down.shape[0]
    columns = pl.ds(pl.multiple_of(me * wide, wide), wide)

    @pl.loop(0, gate.shape[0] // STRIP)
    def _(i):
        rows = pl.ds(pl.multiple_of(i * STRIP, STRIP), STRIP)
        o_gate[rows, columns] = gate[rows, :]
        o_up[rows, columns] = up[rows, :]

    @pl.loop(0, tall // 16)
    def _(i):
        rows = pl.ds(pl.multiple_of(i * 16, 16), 16)
        o_down[pl.ds(pl.multiple_of(me * tall + i * 16, 16), 16), :] = down[rows, :]

    for d in range(1, lines):
        for c in LINE:
            for way, s, cond in (
                (UP, me - d * X, z >= d),
                (DOWN, me + d * X, z + d < lines),
            ):
                arrive(s, c, cond)
                slot = d * n_pieces + c
                send(way, s, c, slot, cond)
                send(SIDE, s, c, slot + (way * lines * n_pieces), cond)

    arrive(partner, PAIR)
    norm_side(partner).wait_recv()

    def norm_pair(way, plane):
        rows = X * widths
        at = widths + way * lines
        return norm_copy(
            norm_rows(plane * rows, rows), plane * rows, rows,
            at + (plane - z) * (1 - 2 * way) * -1, widths + plane, (target(way), w),
        )

    line_slot = 2 * lines * n_pieces
    for d in range(lines):
        for way, plane, cond in (
            (UP, z - d, z >= d),
            (DOWN, z + d, z + d < lines),
        ):
            if d == 0:
                cond = None
            for j in range(X):
                s = me if (d == 0 and j == 0) else (partner if d == 0 else plane * X + j)
                if d > 0:
                    arrive(s, PAIR, cond)
                send(way, s, PAIR, line_slot + d * X + j, cond, from_own=(d == 0 and j == 0))
            full = both(cond, has(way))
            if d > 0:
                when(cond, lambda way=way, plane=plane: norm_pair(way, plane).wait_recv())
            when(full, lambda way=way, plane=plane: norm_pair(way, plane).start())
            sends.append((full, lambda way=way, plane=plane: norm_pair(way, plane).wait_send()))

    for c in LINE:
        arrive(partner, c)
    for d in range(1, lines):
        for c in LINE:
            arrive(partner - d * X, c, z >= d)
            arrive(partner + d * X, c, z + d < lines)
    for k in range(1, widths):
        tile_of(k).wait_send()
    norm_side(me).wait_send()
    for cond, wait in sends:
        when(cond, wait)


def gather_all(shards, widths, gate, up, down, norm):
    lines = shards // X
    n_pieces = len(PIECES)
    any_ = pl.BlockSpec(memory_space=pl.ANY)
    vmem = pl.BlockSpec(memory_space=pltpu.VMEM)
    wide = lambda b: pltpu.VMEM((b.shape[0], shards * b.shape[1]), b.dtype)
    tall = lambda b: pltpu.VMEM((shards * b.shape[0], b.shape[1]), b.dtype)
    return pl.pallas_call(
        functools.partial(gather_kernel, shards, widths),
        out_shape=(
            wide(gate), wide(up), tall(down),
            pltpu.HBM((shards * widths,) + norm.shape[1:], norm.dtype),
        ),
        in_specs=[vmem] * 4,
        out_specs=(vmem,) * 3 + (any_,),
        scratch_shapes=[
            pltpu.SemaphoreType.DMA((3, 2 * lines * n_pieces + lines * X)),
            pltpu.SemaphoreType.DMA((shards * n_pieces,)),
            pltpu.SemaphoreType.DMA((widths + 2 * lines,)),
            pltpu.SemaphoreType.DMA((widths + lines,)),
            pltpu.SemaphoreType.DMA((1,)),
        ],
        compiler_params=pltpu.CompilerParams(collective_id=0, has_side_effects=True, vmem_limit_bytes=16 * 2**20),
    )(gate, up, down, norm)


def write_kernel(gate, up, down, tiles, o_gate, o_up, o_down, o_tiles, sem):
    pairs = ((gate, o_gate), (up, o_up), (down, o_down))
    copies = [pltpu.make_async_copy(a, b, sem.at[i]) for i, (a, b) in enumerate(pairs)]
    for copy in copies:
        copy.start()
    o_tiles[...] = tiles[...]
    for copy in copies:
        copy.wait()


def write_out(gate, up, down, tiles):
    any_ = pl.BlockSpec(memory_space=pl.ANY)
    vmem = pl.BlockSpec(memory_space=pltpu.VMEM)
    return pl.pallas_call(
        write_kernel,
        out_shape=tuple(jax.ShapeDtypeStruct(a.shape, a.dtype) for a in (gate, up, down, tiles)),
        in_specs=[any_] * 3 + [vmem],
        out_specs=(any_,) * 3 + (vmem,),
        scratch_shapes=[pltpu.SemaphoreType.DMA((3,))],
        compiler_params=pltpu.CompilerParams(vmem_limit_bytes=4 * 2**20),
    )(gate, up, down, tiles)


def body(
    shards,
    widths,
    w_gate,
    low_gate,
    high_gate,
    w_up,
    low_up,
    high_up,
    w_down,
    low_down,
    high_down,
    norm_train,
    norm_step,
):
    gate = merged(w_gate, low_gate, high_gate)
    up = merged(w_up, low_up, high_up)
    down = merged(w_down, low_down, high_down)
    gain = norm_train + norm_step
    if shards % X or gate.shape[0] % 128 or down.shape[0] % 256 or gate.shape[0] % STRIP or gain.shape[0] > 128:
        gate, up, down = (
            lax.all_gather(gate, "shard", axis=0, tiled=True),
            lax.all_gather(up, "shard", axis=0, tiled=True),
            lax.all_gather(down, "shard", axis=1, tiled=True),
        )
        gain = lax.all_gather(gain.astype(jnp.bfloat16), ("shard", "width"), axis=0, tiled=True)
        return gate.T, up.T, down.T, gain
    count = gain.shape[0]
    tile = jnp.pad(gain.reshape(1, 1, count), ((0, 0), (0, 7), (0, 128 - count)))
    gate, up, down, tiles = gather_all(shards, widths, gate.T, up.T, down.T, tile)
    gate, up, down, tiles = write_out(gate, up, down, tiles)
    return gate, up, down, tiles[:, 0, :count].reshape(-1).astype(jnp.bfloat16)


def solution(mesh):
    return jax.shard_map(
        functools.partial(body, mesh.shape["shard"], mesh.shape["width"]),
        mesh=mesh,
        in_specs=(
            P("shard", "width"),
            P("shard", None),
            P(None, "width"),
            P("shard", "width"),
            P("shard", None),
            P(None, "width"),
            P("width", "shard"),
            P("width", None),
            P(None, "shard"),
            P(("shard", "width")),
            P(("shard", "width")),
        ),
        out_specs=(P("width", None), P("width", None), P(None, "width"), P()),
        check_vma=False,
    )
```

```python
import functools

import jax
import jax.numpy as jnp
from jax import lax
from jax.experimental import pallas as pl
from jax.experimental.pallas import tpu as pltpu
from jax.sharding import PartitionSpec as P

mix_rate = 2.0
MESH = pl.DeviceIdType.MESH
X = 2


def merged(w, low, high):
    fresh = w.astype(jnp.float32) + mix_rate * jnp.dot(
        low, high, preferred_element_type=jnp.float32
    )
    return fresh.astype(jnp.bfloat16)


PIECES = ((0, 0), (1, 0), (2, 0), (0, 1), (1, 1), (2, 1))
LINE = tuple(range(len(PIECES) - 1))
PAIR = len(PIECES) - 1
UP, DOWN, SIDE = 0, 1, 2
STRIP = 128


def gather_kernel(
    shards, widths, gate, up, down, norm, o_gate, o_up, o_down, o_norm,
    send_sem, recv_sem, norm_send, norm_recv, own_sem,
):
    lines = shards // X
    me, w = lax.axis_index("shard"), lax.axis_index("width")
    z, x = me // X, me % X
    partner = z * X + (1 - x)
    blocks, outs = (gate, up, down), (o_gate, o_up, o_down)
    n_pieces = len(PIECES)

    def own(c):
        t, h = PIECES[c]
        ref = blocks[t]
        if t < 2:
            half = ref.shape[0] // 2
            return ref.at[pl.ds(h * half, half), :]
        half = ref.shape[1] // 2
        return ref.at[:, pl.ds(h * half, half)]

    def place(s, c):
        t, h = PIECES[c]
        ref, out = blocks[t], outs[t]
        if t < 2:
            half, wide = ref.shape[0] // 2, ref.shape[1]
            return out.at[pl.ds(h * half, half), pl.ds(pl.multiple_of(s * wide, wide), wide)]
        half, tall = ref.shape[1] // 2, ref.shape[0]
        return out.at[pl.ds(pl.multiple_of(s * tall, tall), tall), pl.ds(h * half, half)]

    def target(way):
        return {UP: me + X, DOWN: me - X, SIDE: partner}[way]

    sends = []

    def when(conds, fn):
        if conds is None:
            fn()
        else:
            pl.when(conds)(fn)

    def has(way):
        return {UP: z + 1 < lines, DOWN: z > 0, SIDE: None}[way]

    def both(a, b):
        if a is None:
            return b
        if b is None:
            return a
        return jnp.logical_and(a, b)

    def send(way, s, c, slot, cond, from_own=False):
        def make():
            return pltpu.make_async_remote_copy(
                src_ref=own(c) if from_own else place(s, c),
                dst_ref=place(s, c),
                send_sem=send_sem.at[way, slot],
                recv_sem=recv_sem.at[s * n_pieces + c],
                device_id=(target(way), w),
                device_id_type=MESH,
            )

        full = both(cond, has(way))
        when(full, lambda: make().start())
        sends.append((full, lambda: make().wait_send()))

    def arrive(s, c, cond=None):
        when(
            cond,
            lambda: pltpu.make_async_remote_copy(
                src_ref=place(s, c),
                dst_ref=place(s, c),
                send_sem=send_sem.at[0, 0],
                recv_sem=recv_sem.at[s * n_pieces + c],
                device_id=(partner, w),
                device_id_type=MESH,
            ).wait_recv(),
        )

    def norm_rows(first, count):
        return o_norm.at[pl.ds(first, count)]

    def norm_copy(src, first, count, sem, rsem, dev):
        return pltpu.make_async_remote_copy(
            src_ref=src, dst_ref=norm_rows(first, count), send_sem=norm_send.at[sem],
            recv_sem=norm_recv.at[rsem], device_id=dev, device_id_type=MESH,
        )

    barrier = pltpu.get_barrier_semaphore()
    peers = [lax.rem(w + k, widths) for k in range(1, widths)]
    for p in peers:
        pl.semaphore_signal(barrier, inc=1, device_id=(me, p), device_id_type=MESH)
    for way in (UP, DOWN, SIDE):
        when(
            has(way),
            lambda way=way: pl.semaphore_signal(
                barrier, inc=1, device_id=(target(way), w), device_id_type=MESH
            ),
        )
    inner = jnp.logical_and(z > 0, z + 1 < lines)
    pl.when(inner)(lambda: pl.semaphore_wait(barrier, widths + 2))
    ends = widths + (1 if lines > 1 else 0)
    pl.when(jnp.logical_not(inner))(lambda: pl.semaphore_wait(barrier, ends))

    send(SIDE, me, PAIR, PAIR, None, from_own=True)
    for c in LINE:
        send(UP, me, c, c, None, from_own=True)
        send(DOWN, me, c, c, None, from_own=True)
        send(SIDE, me, c, c, None, from_own=True)
    norm_own = pltpu.make_async_copy(norm, norm_rows(me * widths + w, 1), own_sem.at[0])
    norm_own.start()
    tile_of = lambda k: norm_copy(norm, me * widths + w, 1, k - 1, k - 1, (me, peers[k - 1]))
    for k in range(1, widths):
        tile_of(k).start()
    norm_own.wait()
    for k in range(1, widths):
        source = lax.rem(w + widths - k, widths)
        norm_copy(norm, me * widths + source, 1, k - 1, k - 1, (me, peers[k - 1])).wait_recv()
    side_at = widths - 1
    norm_side = lambda s: norm_copy(
        norm_rows(s * widths, widths), s * widths, widths, side_at, side_at, (partner, w)
    )
    norm_side(me).start()

    wide, tall = gate.shape[1], down.shape[0]
    columns = pl.ds(pl.multiple_of(me * wide, wide), wide)

    @pl.loop(0, gate.shape[0] // STRIP)
    def _(i):
        rows = pl.ds(pl.multiple_of(i * STRIP, STRIP), STRIP)
        o_gate[rows, columns] = gate[rows, :]
        o_up[rows, columns] = up[rows, :]

    @pl.loop(0, tall // 16)
    def _(i):
        rows = pl.ds(pl.multiple_of(i * 16, 16), 16)
        o_down[pl.ds(pl.multiple_of(me * tall + i * 16, 16), 16), :] = down[rows, :]

    for d in range(1, lines):
        for c in LINE:
            for way, s, cond in (
                (UP, me - d * X, z >= d),
                (DOWN, me + d * X, z + d < lines),
            ):
                arrive(s, c, cond)
                slot = d * n_pieces + c
                send(way, s, c, slot, cond)
                send(SIDE, s, c, slot + (way * lines * n_pieces), cond)

    arrive(partner, PAIR)
    norm_side(partner).wait_recv()

    def norm_pair(way, plane):
        rows = X * widths
        at = widths + way * lines
        return norm_copy(
            norm_rows(plane * rows, rows), plane * rows, rows,
            at + (plane - z) * (1 - 2 * way) * -1, widths + plane, (target(way), w),
        )

    line_slot = 2 * lines * n_pieces
    for d in range(lines):
        for way, plane, cond in (
            (UP, z - d, z >= d),
            (DOWN, z + d, z + d < lines),
        ):
            if d == 0:
                cond = None
            for j in range(X):
                s = me if (d == 0 and j == 0) else (partner if d == 0 else plane * X + j)
                if d > 0:
                    arrive(s, PAIR, cond)
                send(way, s, PAIR, line_slot + d * X + j, cond, from_own=(d == 0 and j == 0))
            full = both(cond, has(way))
            if d > 0:
                when(cond, lambda way=way, plane=plane: norm_pair(way, plane).wait_recv())
            when(full, lambda way=way, plane=plane: norm_pair(way, plane).start())
            sends.append((full, lambda way=way, plane=plane: norm_pair(way, plane).wait_send()))

    for c in LINE:
        arrive(partner, c)
    for d in range(1, lines):
        for c in LINE:
            arrive(partner - d * X, c, z >= d)
            arrive(partner + d * X, c, z + d < lines)
    for k in range(1, widths):
        tile_of(k).wait_send()
    norm_side(me).wait_send()
    for cond, wait in sends:
        when(cond, wait)


def gather_all(shards, widths, gate, up, down, norm):
    lines = shards // X
    n_pieces = len(PIECES)
    any_ = pl.BlockSpec(memory_space=pl.ANY)
    vmem = pl.BlockSpec(memory_space=pltpu.VMEM)
    wide = lambda b: pltpu.VMEM((b.shape[0], shards * b.shape[1]), b.dtype)
    tall = lambda b: pltpu.VMEM((shards * b.shape[0], b.shape[1]), b.dtype)
    return pl.pallas_call(
        functools.partial(gather_kernel, shards, widths),
        out_shape=(
            wide(gate), wide(up), tall(down),
            pltpu.HBM((shards * widths,) + norm.shape[1:], norm.dtype),
        ),
        in_specs=[vmem] * 4,
        out_specs=(vmem,) * 3 + (any_,),
        scratch_shapes=[
            pltpu.SemaphoreType.DMA((3, 2 * lines * n_pieces + lines * X)),
            pltpu.SemaphoreType.DMA((shards * n_pieces,)),
            pltpu.SemaphoreType.DMA((widths + 2 * lines,)),
            pltpu.SemaphoreType.DMA((widths + lines,)),
            pltpu.SemaphoreType.DMA((1,)),
        ],
        compiler_params=pltpu.CompilerParams(collective_id=0, has_side_effects=True, vmem_limit_bytes=16 * 2**20),
    )(gate, up, down, norm)


def write_kernel(gate, up, down, tiles, o_gate, o_up, o_down, o_tiles, sem):
    pairs = ((gate, o_gate), (up, o_up), (down, o_down))
    copies = [pltpu.make_async_copy(a, b, sem.at[i]) for i, (a, b) in enumerate(pairs)]
    for copy in copies:
        copy.start()
    o_tiles[...] = tiles[...]
    for copy in copies:
        copy.wait()


def write_out(gate, up, down, tiles):
    any_ = pl.BlockSpec(memory_space=pl.ANY)
    vmem = pl.BlockSpec(memory_space=pltpu.VMEM)
    return pl.pallas_call(
        write_kernel,
        out_shape=tuple(jax.ShapeDtypeStruct(a.shape, a.dtype) for a in (gate, up, down, tiles)),
        in_specs=[any_] * 3 + [vmem],
        out_specs=(any_,) * 3 + (vmem,),
        scratch_shapes=[pltpu.SemaphoreType.DMA((3,))],
        compiler_params=pltpu.CompilerParams(vmem_limit_bytes=4 * 2**20),
    )(gate, up, down, tiles)


def merge_kernel(*refs):
    ins, outs = refs[:9], refs[9:]
    for t in range(3):
        w, low, high = ins[3 * t : 3 * t + 3]
        delta = lax.dot_general(
            high[...], low[...], (((0,), (0,)), ((), ())), preferred_element_type=jnp.float32
        )
        outs[t][...] = (w[...].astype(jnp.float32).T + mix_rate * delta).astype(jnp.bfloat16)


def merge_all(strip, *arrays):
    wg, lg, hg, wu, lu, hu, wd, ld, hd = arrays
    rank = lg.shape[1]

    def first(w):
        tall = w.shape[0]
        return [
            pl.BlockSpec((tall, strip), lambda i: (0, i)),
            pl.BlockSpec((rank, tall), lambda i: (0, 0)),
            pl.BlockSpec((rank, strip), lambda i: (0, i)),
        ]

    wide = wd.shape[1]
    last = [
        pl.BlockSpec((strip, wide), lambda i: (i, 0)),
        pl.BlockSpec((rank, strip), lambda i: (0, i)),
        pl.BlockSpec((rank, wide), lambda i: (0, 0)),
    ]
    return pl.pallas_call(
        merge_kernel,
        grid=(wg.shape[1] // strip,),
        out_shape=tuple(jax.ShapeDtypeStruct(w.shape[::-1], w.dtype) for w in (wg, wu, wd)),
        in_specs=first(wg) + first(wu) + last,
        out_specs=(
            pl.BlockSpec((strip, wg.shape[0]), lambda i: (i, 0)),
            pl.BlockSpec((strip, wu.shape[0]), lambda i: (i, 0)),
            pl.BlockSpec((wide, strip), lambda i: (0, i)),
        ),
        compiler_params=pltpu.CompilerParams(vmem_limit_bytes=16 * 2**20),
    )(wg, lg.T, hg, wu, lu.T, hu, wd, ld.T, hd)


def body(
    shards,
    widths,
    w_gate,
    low_gate,
    high_gate,
    w_up,
    low_up,
    high_up,
    w_down,
    low_down,
    high_down,
    norm_train,
    norm_step,
):
    gate = merged(w_gate, low_gate, high_gate)
    up = merged(w_up, low_up, high_up)
    down = merged(w_down, low_down, high_down)
    gain = norm_train + norm_step
    if shards % X or gate.shape[0] % 128 or down.shape[0] % 256 or gate.shape[1] % 256 or down.shape[0] != gate.shape[1] or gain.shape[0] > 128:
        gate, up, down = (
            lax.all_gather(gate, "shard", axis=0, tiled=True),
            lax.all_gather(up, "shard", axis=0, tiled=True),
            lax.all_gather(down, "shard", axis=1, tiled=True),
        )
        gain = lax.all_gather(gain.astype(jnp.bfloat16), ("shard", "width"), axis=0, tiled=True)
        return gate.T, up.T, down.T, gain
    count = gain.shape[0]
    tile = jnp.pad(gain.reshape(1, 1, count), ((0, 0), (0, 7), (0, 128 - count)))
    gate, up, down = merge_all(
        256, w_gate, low_gate, high_gate, w_up, low_up, high_up, w_down, low_down, high_down
    )
    gate, up, down, tiles = gather_all(shards, widths, gate, up, down, tile)
    gate, up, down, tiles = write_out(gate, up, down, tiles)
    return gate, up, down, tiles[:, 0, :count].reshape(-1).astype(jnp.bfloat16)


def solution(mesh):
    return jax.shard_map(
        functools.partial(body, mesh.shape["shard"], mesh.shape["width"]),
        mesh=mesh,
        in_specs=(
            P("shard", "width"),
            P("shard", None),
            P(None, "width"),
            P("shard", "width"),
            P("shard", None),
            P(None, "width"),
            P("width", "shard"),
            P("width", None),
            P(None, "shard"),
            P(("shard", "width")),
            P(("shard", "width")),
        ),
        out_specs=(P("width", None), P("width", None), P(None, "width"), P()),
        check_vma=False,
    )
```
